8 devices in a mesh: dp: 2 (over y, z), tp: 4 (over x, core).
Axes of the slice: x: 2, y: 2, z: 1, core: 2. Of those that a mesh axis runs over, the one named last changes fastest.
Arguments:
- x: bfloat16 [4096, 2048], P('dp'), parts along dimension 0
- dy: bfloat16 [4096, 2048], P('dp'), parts along dimension 0
- gate: bfloat16 [4096, 6144], P('dp', 'tp'), parts along dimension 0
- up: bfloat16 [4096, 6144], P('dp', 'tp'), parts along dimension 0
- w_gate: bfloat16 [2048, 6144], P(None, 'tp')
- w_up: bfloat16 [2048, 6144], P(None, 'tp')
- w_down: bfloat16 [6144, 2048], P('tp')
Outputs:
- output 1: bfloat16 [4096, 2048], P('dp'), parts along dimension 0
- output 2: bfloat16 [4096, 6144], P('dp', 'tp'), parts along dimension 0
- output 3: bfloat16 [4096, 6144], P('dp', 'tp'), parts along dimension 0
- output 4: bfloat16 [12288, 2048], P(('dp', 'tp')), parts along dimension 0
There are 2 independent parts. The reference program is written for one: setup_inputs(seed, part) draws one part's arguments, and reference() takes and returns one part's arrays. A program takes and returns all parts, laid end to end along the dimension named above; an argument that names none is the same for every part.
All inputs are finite; a program needn't handle non-finite values.
Results may differ from the reference program's by a relative error of at most 0.012.
Values are sent between devices in bfloat16 or wider.
A program may use at most 2 GiB of HBM per device.

```python
import jax
import jax.numpy as jnp

ROWS = 2048
D = 2048
FF = 6144


def act(gate, up):
    return jax.nn.silu(gate) * up


def setup_inputs(seed: int = 0, part: int = 0) -> dict:
    kx, ky, ka, kb, kg, ku, kd = jax.random.split(jax.random.key(seed), 7)
    kx, ky, ka, kb = (jax.random.fold_in(k, part) for k in (kx, ky, ka, kb))
    drawn = {
        "x": jax.random.normal(kx, (ROWS, D), jnp.float32),
        "dy": jax.random.normal(ky, (ROWS, D), jnp.float32),
        "gate": jax.random.normal(ka, (ROWS, FF), jnp.float32),
        "up": jax.random.normal(kb, (ROWS, FF), jnp.float32),
        "w_gate": jax.random.normal(kg, (D, FF), jnp.float32) * D**-0.5,
        "w_up": jax.random.normal(ku, (D, FF), jnp.float32) * D**-0.5,
        "w_down": jax.random.normal(kd, (FF, D), jnp.float32) * FF**-0.5,
    }
    return {k: v.astype(jnp.bfloat16) for k, v in drawn.items()}


def reference(x, dy, gate, up, w_gate, w_up, w_down):
    hidden, back = jax.vjp(act, gate.astype(jnp.float32), up.astype(jnp.float32))
    d_hidden = jnp.dot(dy, w_down.T, preferred_element_type=jnp.float32)
    d_gate, d_up = (g.astype(jnp.bfloat16) for g in back(d_hidden))
    dx = jnp.dot(d_gate, w_gate.T, preferred_element_type=jnp.float32) + jnp.dot(d_up, w_up.T, preferred_element_type=jnp.float32)
    dw_gate = jnp.dot(x.T, d_gate, preferred_element_type=jnp.float32)
    dw_up = jnp.dot(x.T, d_up, preferred_element_type=jnp.float32)
    dw_down = jnp.dot(hidden.astype(jnp.bfloat16).T, dy, preferred_element_type=jnp.float32)
    return tuple(g.astype(jnp.bfloat16) for g in (dx, dw_gate, dw_up, dw_down))
```

```python
import functools

import jax
import jax.numpy as jnp
from jax import lax
from jax.experimental import pallas as pl
from jax.experimental.pallas import tpu as pltpu
from jax.sharding import PartitionSpec as P

MESH = pl.DeviceIdType.MESH
BF16, F32 = jnp.bfloat16, jnp.float32
ANY = pl.BlockSpec(memory_space=pl.ANY)

ROWS, D, FF = 2048, 2048, 1536
HALF = D // 2
RB = 256
NB = ROWS // RB
HB = RB // 2
NX = 7
PARTS = ((7, 11), (11, 14), (14, 16))
TILE = 512

CHIPS = [(0, 2), (2, 0), (1, 3), (3, 1)]
CORES = [(0, 1), (1, 0), (2, 3), (3, 2)]


def dot(a, b, dims):
    return lax.dot_general(a, b, (dims, ((), ())), preferred_element_type=F32)


def term_kernel(
    dy, gate, up, wd, wg, wu,
    dg_o, du_o, h_o, dxp, *refs,
):
    outs, refs = refs[: len(PARTS)], refs[len(PARTS) :]
    (
        wd_v, wgu_v, dy_v, ga_v, up_v, dgu_v, h_v, yours, mine, theirs, s_v, q_v, f_v,
        w_sem, in_sem, out_sem, cs_sem, cr_sem, xs_sem, xr_sem, gs_sem, gr_sem, f_sem, s_sem,
    ) = refs
    me = lax.axis_index("tp")
    core = lax.rem(me, 2)
    partner = me + 1 - 2 * core
    across = lax.rem(me + 2, 4)

    def rows(i):
        return pl.ds(pl.multiple_of(i * RB, RB), RB)

    def loads(i, slot):
        return [
            pltpu.make_async_copy(src.at[rows(i)], dst.at[slot], in_sem.at[n, slot])
            for n, (src, dst) in enumerate(((dy, dy_v), (gate, ga_v), (up, up_v)))
        ]

    def stores(i, slot):
        return [
            pltpu.make_async_copy(dgu_v.at[slot, :, pl.ds(0, FF)], dg_o.at[rows(i)], out_sem.at[0, slot]),
            pltpu.make_async_copy(dgu_v.at[slot, :, pl.ds(FF, FF)], du_o.at[rows(i)], out_sem.at[1, slot]),
            pltpu.make_async_copy(h_v.at[slot], h_o.at[rows(i)], out_sem.at[2, slot]),
        ]

    def swap(i):
        return pltpu.make_async_remote_copy(
            yours.at[i], theirs.at[i], cs_sem.at[i], cr_sem.at[i], device_id={"tp": partner}, device_id_type=MESH
        )

    def cross(k):
        return pltpu.make_async_remote_copy(
            s_v.at[k], q_v.at[k], xs_sem.at[k], xr_sem.at[k], device_id={"tp": across}, device_id_type=MESH
        )

    def finished(k):
        return dxp.at[core, pl.ds(pl.multiple_of(k * HB, HB), HB)]

    def keep(k):
        return pltpu.make_async_copy(f_v.at[k], finished(k), f_sem.at[k])

    def give(k):
        return pltpu.make_async_remote_copy(
            f_v.at[k], finished(k), gs_sem.at[k], gr_sem.at[k], device_id={"tp": partner}, device_id_type=MESH
        )

    def hand_on(k):
        for out, (first, last) in zip(outs, PARTS):
            if first <= k < last:
                return pltpu.make_async_copy(s_v.at[k], out.at[pl.ds((k - first) * HB, HB)], s_sem.at[k])

    weights = [
        pltpu.make_async_copy(wd, wd_v, w_sem.at[0]),
        pltpu.make_async_copy(wg, wgu_v.at[:, pl.ds(0, FF)], w_sem.at[1]),
        pltpu.make_async_copy(wu, wgu_v.at[:, pl.ds(FF, FF)], w_sem.at[2]),
    ]
    for copy in loads(0, 0):
        copy.start()
    for copy in weights:
        copy.start()

    barrier = pltpu.get_barrier_semaphore()
    for other in (partner, across):
        pl.semaphore_signal(barrier, inc=1, device_id={"tp": other}, device_id_type=MESH)
    pl.semaphore_wait(barrier, 2)

    def finish(k):
        cross(k).wait_recv()
        f_v[k] = (s_v[k].astype(F32) + q_v[k].astype(F32)).astype(BF16)
        keep(k).start()
        give(k).start()

    def step(i, carry):
        slot = lax.rem(i, 2)
        for copy in loads(i, slot):
            copy.wait()

        @pl.when(i + 1 < NB)
        def _():
            for copy in loads(i + 1, 1 - slot):
                copy.start()

        @pl.when(i == 0)
        def _():
            weights[0].wait()

        @pl.when(i >= 2)
        def _():
            for copy in stores(i - 2, slot):
                copy.wait()

        for t in range(FF // TILE):
            cols = pl.ds(t * TILE, TILE)
            d_hidden = dot(dy_v[slot], wd_v[cols, :], ((1,), (1,)))
            g, u = ga_v[slot, :, cols].astype(F32), up_v[slot, :, cols].astype(F32)
            sig = jax.nn.sigmoid(g)
            silu = g * sig
            h_v[slot, :, cols] = (silu * u).astype(BF16)
            dgu_v[slot, :, cols] = (d_hidden * u * (sig + silu * (1.0 - sig))).astype(BF16)
            dgu_v[slot, :, pl.ds(FF + t * TILE, TILE)] = (d_hidden * silu).astype(BF16)
        for copy in stores(i, slot):
            copy.start()

        @pl.when(i == 0)
        def _():
            weights[1].wait()
            weights[2].wait()

        def term(half, t):
            at = pl.multiple_of(half * HALF + t * TILE, TILE)
            return dot(dgu_v[slot], wgu_v[pl.ds(at, TILE), :], ((1,), (1,)))

        for t in range(HALF // TILE):
            yours[i, :, pl.ds(t * TILE, TILE)] = term(1 - core, t).astype(BF16)
        swap(i).start()
        for t in range(HALF // TILE):
            mine[:, pl.ds(t * TILE, TILE)] = term(core, t)
        swap(i).wait_recv()
        for n in range(2):
            part = pl.ds(n * HB, HB)
            s_v[2 * i + n] = (mine[part, :] + theirs[i, part, :].astype(F32)).astype(BF16)

            @pl.when(2 * i + n < NX)
            def _():
                cross(2 * i + n).start()

        for k in range(NX, 2 * NB):

            @pl.when(i == k // 2)
            def _():
                hand_on(k).start()

        @pl.when(jnp.logical_and(i >= 2, i - 2 < NX))
        def _():
            finish(i - 2)

        return carry

    lax.fori_loop(0, NB, step, 0)
    for k in range(NB - 2, NX):
        finish(k)
    for i in (NB - 2, NB - 1):
        for copy in stores(i, i % 2):
            copy.wait()
    for i in range(NB):
        swap(i).wait_send()
    for k in range(NX):
        cross(k).wait_send()
        keep(k).wait()
        give(k).wait()
    for k in range(NX, 2 * NB):
        hand_on(k).wait()


def terms(dy, gate, up, w_down, w_gate, w_up):
    hidden = jax.ShapeDtypeStruct((ROWS, FF), BF16)
    return pl.pallas_call(
        term_kernel,
        name="terms",
        out_shape=(
            hidden,
            hidden,
            hidden,
            jax.ShapeDtypeStruct((2, NX * HB, HALF), BF16),
            *(jax.ShapeDtypeStruct(((b - a) * HB, HALF), BF16) for a, b in PARTS),
        ),
        in_specs=[ANY] * 6,
        out_specs=(ANY,) * (4 + len(PARTS)),
        scratch_shapes=[
            pltpu.VMEM((FF, D), BF16),
            pltpu.VMEM((D, 2 * FF), BF16),
            pltpu.VMEM((2, RB, D), BF16),
            pltpu.VMEM((2, RB, FF), BF16),
            pltpu.VMEM((2, RB, FF), BF16),
            pltpu.VMEM((2, RB, 2 * FF), BF16),
            pltpu.VMEM((2, RB, FF), BF16),
            pltpu.VMEM((NB, RB, HALF), BF16),
            pltpu.VMEM((RB, HALF), F32),
            pltpu.VMEM((NB, RB, HALF), BF16),
            pltpu.VMEM((2 * NB, HB, HALF), BF16),
            pltpu.VMEM((NX, HB, HALF), BF16),
            pltpu.VMEM((NX, HB, HALF), BF16),
            pltpu.SemaphoreType.DMA((3,)),
            pltpu.SemaphoreType.DMA((3, 2)),
            pltpu.SemaphoreType.DMA((3, 2)),
            pltpu.SemaphoreType.DMA((NB,)),
            pltpu.SemaphoreType.DMA((NB,)),
            pltpu.SemaphoreType.DMA((NX,)),
            pltpu.SemaphoreType.DMA((NX,)),
            pltpu.SemaphoreType.DMA((NX,)),
            pltpu.SemaphoreType.DMA((NX,)),
            pltpu.SemaphoreType.DMA((NX,)),
            pltpu.SemaphoreType.DMA((2 * NB,)),
        ],
        cost_estimate=pl.CostEstimate(flops=6 * ROWS * D * FF, bytes_accessed=60 * 2**20, transcendentals=ROWS * FF),
        compiler_params=pltpu.CompilerParams(collective_id=0, has_side_effects=True, vmem_limit_bytes=60 * 2**20),
    )(dy, gate, up, w_down, w_gate, w_up)


def weight_kernel(x, h, dg, du, dy, dxp, dwg, dwu, dwd, dx, dg_v, du_v, dy_v, dx_v, sem, i_sem, o_sem):
    j = pl.program_id(0)
    whole = [
        pltpu.make_async_copy(src, dst, sem.at[n]) for n, (src, dst) in enumerate(((dg, dg_v), (du, du_v), (dy, dy_v)))
    ]
    takes = [
        pltpu.make_async_copy(dxp.at[c], dx_v.at[:, pl.ds(c * HALF, HALF)], i_sem.at[c]) for c in range(2)
    ]
    puts = pltpu.make_async_copy(dx_v, dx.at[pl.ds(0, NX * HB)], o_sem)

    @pl.when(j == 0)
    def _():
        for copy in (*whole, *takes):
            copy.start()
        whole[0].wait()

    @pl.when(j == 1)
    def _():
        for copy in takes:
            copy.wait()
        puts.start()

    dwg[...] = dot(x[...], dg_v[...], ((0,), (0,))).astype(BF16)

    @pl.when(j == 0)
    def _():
        whole[1].wait()

    dwu[...] = dot(x[...], du_v[...], ((0,), (0,))).astype(BF16)

    @pl.when(j == 0)
    def _():
        whole[2].wait()

    dwd[...] = dot(h[...], dy_v[...], ((0,), (0,))).astype(BF16)

    @pl.when(j == pl.num_programs(0) - 1)
    def _():
        puts.wait()


def weights(x, h, dg, du, dy, dxp):
    n = 4
    bx, bh = D // n, FF // n
    return pl.pallas_call(
        weight_kernel,
        name="weights",
        grid=(n,),
        out_shape=(
            jax.ShapeDtypeStruct((D, FF), BF16),
            jax.ShapeDtypeStruct((D, FF), BF16),
            jax.ShapeDtypeStruct((FF, D), BF16),
            jax.ShapeDtypeStruct((ROWS, D), BF16),
        ),
        in_specs=[pl.BlockSpec((ROWS, bx), lambda j: (0, j)), pl.BlockSpec((ROWS, bh), lambda j: (0, j)), ANY, ANY, ANY, ANY],
        out_specs=(
            pl.BlockSpec((bx, FF), lambda j: (j, 0)),
            pl.BlockSpec((bx, FF), lambda j: (j, 0)),
            pl.BlockSpec((bh, D), lambda j: (j, 0)),
            ANY,
        ),
        scratch_shapes=[
            pltpu.VMEM((ROWS, FF), BF16),
            pltpu.VMEM((ROWS, FF), BF16),
            pltpu.VMEM((ROWS, D), BF16),
            pltpu.VMEM((NX * HB, D), BF16),
            pltpu.SemaphoreType.DMA((3,)),
            pltpu.SemaphoreType.DMA((2,)),
            pltpu.SemaphoreType.DMA,
        ],
        cost_estimate=pl.CostEstimate(flops=6 * ROWS * D * FF, bytes_accessed=60 * 2**20, transcendentals=0),
        compiler_params=pltpu.CompilerParams(vmem_limit_bytes=60 * 2**20),
    )(x, h, dg, du, dy, dxp)


def place_kernel(f, g, dx, out):
    core = lax.rem(lax.axis_index("tp"), 2)
    for c in range(2):

        @pl.when(core == c)
        def _():
            out[:, c * HALF : (c + 1) * HALF] = f[...]
            out[:, (1 - c) * HALF : (2 - c) * HALF] = g[...]


def place(dx, f, g, first):
    n = f.shape[0] // HB
    half = pl.BlockSpec((HB, HALF), lambda j: (j, 0))
    return pl.pallas_call(
        place_kernel,
        name="place",
        grid=(n,),
        out_shape=jax.ShapeDtypeStruct(dx.shape, BF16),
        in_specs=[half, half, ANY],
        out_specs=pl.BlockSpec((HB, D), lambda j: (first + j, 0)),
        input_output_aliases={2: 0},
        cost_estimate=pl.CostEstimate(flops=n * HB * D, bytes_accessed=n * HB * D * 4, transcendentals=0),
    )(f, g, dx)


def solution(mesh):
    def step(x, dy, gate, up, w_gate, w_up, w_down):
        dg, du, h, dxp, *parts = terms(dy, gate, up, w_down, w_gate, w_up)
        theirs = [lax.ppermute(s, "tp", CHIPS) for s in parts]
        dw_gate, dw_up, dw_down, dx = weights(x, h, dg, du, dy, dxp)
        dx, *theirs = lax.optimization_barrier((dx, *theirs))
        for (first, _), s, q in zip(PARTS, parts, theirs):
            f = (s.astype(F32) + q.astype(F32)).astype(BF16)
            dx = place(dx, f, lax.ppermute(f, "tp", CORES), first)
        return dx, dw_gate, dw_up, dw_down

    tokens, columns, rows = P("dp", None), P(None, "tp"), P("tp", None)
    return jax.shard_map(
        step,
        mesh=mesh,
        in_specs=(tokens, tokens, P("dp", "tp"), P("dp", "tp"), columns, columns, rows),
        out_specs=(tokens, P("dp", "tp"), P("dp", "tp"), P(("dp", "tp"), None)),
        check_vma=False,
    )
```

```python
import functools

import jax
import jax.numpy as jnp
from jax import lax
from jax.experimental import pallas as pl
from jax.experimental.pallas import tpu as pltpu
from jax.sharding import PartitionSpec as P


MESH = pl.DeviceIdType.MESH
BF16, F32 = jnp.bfloat16, jnp.float32
ANY = pl.BlockSpec(memory_space=pl.ANY)
MIB = 2**20

ROWS, D, FF = 2048, 2048, 1536
HALF = D // 2
RB = 256
NB = ROWS // RB
HB = RB // 2
NX = 10
PARTS = ((10, 15), (15, 16))
TILE = 512
Q = 512
NQ = HALF // Q
BX = 512
NJ = D // BX
BH = FF // NJ

CHIPS = [(0, 2), (2, 0), (1, 3), (3, 1)]
CORES = [(0, 1), (1, 0), (2, 3), (3, 2)]


def dot(a, b, dims):
    return lax.dot_general(a, b, (dims, ((), ())), preferred_element_type=F32)


def to(axis, index):
    return dict(device_id={axis: index}, device_id_type=MESH)


def term_kernel(dy, gate, up, wd, wg, wu, x, du_o, h_o, dwg_o, dxp, *refs):
    n = len(PARTS)
    own_o, both_o, refs = refs[:n], refs[n : 2 * n], refs[2 * n :]
    (
        wd_v, wgu_v, dy_v, ga_v, up_v, dgu_v, h_v, dg_v, x_v, yours, mine, theirs, s_v, q_v, f_v,
        yours_0, theirs_0, s_0, q_0, f_0,
        wd_sem, wg_sem, in_sem, out_sem, x_sem, dw_sem, cs_sem, cr_sem, xs_sem, xr_sem, gs_sem, gr_sem, f_sem,
        own_sem, both_sem, bs_sem, br_sem, cs0, cr0, xs0, xr0, gs0, gr0, f0,
    ) = refs
    me = lax.axis_index("tp")
    core = lax.rem(me, 2)
    partner = me + 1 - 2 * core
    across = lax.rem(me + 2, 4)

    def rows(i):
        return pl.ds(pl.multiple_of(i * RB, RB), RB)

    def loads(i, slot):
        return [
            pltpu.make_async_copy(src.at[rows(i)], dst.at[slot], in_sem.at[n, slot])
            for n, (src, dst) in enumerate(((dy, dy_v), (gate, ga_v), (up, up_v)))
        ]

    def stores(i, slot):
        return [
            pltpu.make_async_copy(dgu_v.at[slot, :, pl.ds(FF, FF)], du_o.at[rows(i)], out_sem.at[0, slot]),
            pltpu.make_async_copy(h_v.at[slot], h_o.at[rows(i)], out_sem.at[1, slot]),
        ]

    def swap(i):
        return pltpu.make_async_remote_copy(
            yours.at[i], theirs.at[i], cs_sem.at[i], cr_sem.at[i], **to("tp", partner)
        )

    def cross(k):
        return pltpu.make_async_remote_copy(s_v.at[k], q_v.at[k], xs_sem.at[k], xr_sem.at[k], **to("tp", across))

    def finished(k):
        return dxp.at[core, pl.ds(pl.multiple_of(k * HB, HB), HB)]

    def keep(k):
        return pltpu.make_async_copy(f_v.at[k], finished(k), f_sem.at[k])

    def give(k):
        return pltpu.make_async_remote_copy(f_v.at[k], finished(k), gs_sem.at[k], gr_sem.at[k], **to("tp", partner))

    def swap_0(q):
        return pltpu.make_async_remote_copy(yours_0.at[q], theirs_0.at[q], cs0.at[q], cr0.at[q], **to("tp", partner))

    def cross_0(q):
        return pltpu.make_async_remote_copy(s_0.at[q], q_0.at[q], xs0.at[q], xr0.at[q], **to("tp", across))

    def finished_0(q):
        return dxp.at[core, pl.ds(0, RB), pl.ds(pl.multiple_of(q * Q, Q), Q)]

    def keep_0(q):
        return pltpu.make_async_copy(f_0.at[q], finished_0(q), f0.at[q])

    def give_0(q):
        return pltpu.make_async_remote_copy(f_0.at[q], finished_0(q), gs0.at[q], gr0.at[q], **to("tp", partner))

    def hand_on(k):
        for own, both, (first, last) in zip(own_o, both_o, PARTS):
            if first <= k < last:
                at, j = pl.ds((k - first) * HB, HB), k - NX
                return (
                    pltpu.make_async_copy(s_v.at[k], own.at[at], own_sem.at[j]),
                    pltpu.make_async_copy(s_v.at[k], both.at[core, at], both_sem.at[j]),
                    pltpu.make_async_remote_copy(
                        s_v.at[k], both.at[core, at], bs_sem.at[j], br_sem.at[j], **to("tp", partner)
                    ),
                )

    def wd_load(t):
        at = pl.ds(t * TILE, TILE)
        return pltpu.make_async_copy(wd.at[at], wd_v.at[at], wd_sem.at[t])

    def wgu_at(half, t, size):
        return pl.ds(pl.multiple_of(half * HALF + t * size, size), size)

    def wgu_load(n, half, t):
        at = wgu_at(half, t, Q)
        return [
            pltpu.make_async_copy(w.at[at], wgu_v.at[at, pl.ds(m * FF, FF)], wg_sem.at[n, t, m])
            for m, w in enumerate((wg, wu))
        ]

    def x_at(j):
        return x_v if j == 0 else wgu_v.at[:, pl.ds((j - 1) * BX, BX)]

    def x_load(j):
        return pltpu.make_async_copy(x.at[:, pl.ds(j * BX, BX)], x_at(j), x_sem.at[j])

    def dw_at(j):
        return wgu_v.at[pl.ds(j * BX, BX), pl.ds(FF, FF)]

    def dw_store(j):
        return pltpu.make_async_copy(dw_at(j), dwg_o.at[pl.ds(j * BX, BX)], dw_sem.at[j])

    def start(copies):
        for copy in copies:
            copy.start()

    def wait(copies):
        for copy in copies:
            copy.wait()

    first_loads = loads(0, 0)
    start([first_loads[0], wd_load(0)])
    start([*first_loads[1:], wd_load(1)])

    barrier = pltpu.get_barrier_semaphore()
    for other in (partner, across):
        pl.semaphore_signal(barrier, inc=1, **to("tp", other))
    pl.semaphore_wait(barrier, 2)

    def finish(k):
        cross(k).wait_recv()
        f_v[k] = (s_v[k].astype(F32) + q_v[k].astype(F32)).astype(BF16)
        keep(k).start()
        give(k).start()

    def finish_0(q):
        cross_0(q).wait_recv()
        f_0[q] = (s_0[q].astype(F32) + q_0[q].astype(F32)).astype(BF16)
        keep_0(q).start()
        give_0(q).start()

    def hidden(i, slot, t):
        cols = pl.ds(t * TILE, TILE)
        d_hidden = dot(dy_v[slot], wd_v[cols, :], ((1,), (1,)))
        if isinstance(i, int) and t == 0:
            wait(first_loads[1:])
        g, u = ga_v[slot, :, cols].astype(F32), up_v[slot, :, cols].astype(F32)
        sig = jax.nn.sigmoid(g)
        silu = g * sig
        d_gate = (d_hidden * u * (sig + silu * (1.0 - sig))).astype(BF16)
        h_v[slot, :, cols] = (silu * u).astype(BF16)
        dgu_v[slot, :, cols] = d_gate
        dg_v[rows(i), cols] = d_gate
        dgu_v[slot, :, pl.ds(FF + t * TILE, TILE)] = (d_hidden * silu).astype(BF16)

    def term(slot, half, t, size):
        return dot(dgu_v[slot], wgu_v[wgu_at(half, t, size), :], ((1,), (1,)))

    def first_block():
        wait([first_loads[0], wd_load(0)])
        start([wd_load(2)])
        hidden(0, 0, 0)
        wait([wd_load(1)])
        halves = (1 - core, core)
        order = [(n, half, q) for q in range(NQ) for n, half in enumerate(halves)]
        start(wgu_load(*order[0]))
        hidden(0, 0, 1)
        wait([wd_load(2)])
        start(wgu_load(*order[1]))
        start(wgu_load(*order[2]))
        hidden(0, 0, 2)

        def add(q):
            swap_0(q).wait_recv()
            at = pl.ds(q * Q, Q)
            s_0[q] = (mine[:, at] + theirs_0[q].astype(F32)).astype(BF16)
            cross_0(q).start()

        for at, (n, half, q) in enumerate(order):
            wait(wgu_load(n, half, q))
            if at + 3 < len(order):
                start(wgu_load(*order[at + 3]))
            elif at + 3 == len(order):
                start(loads(1, 1))
            elif at + 3 == len(order) + 1:
                start(stores(0, 0))
            got = term(0, half, q, Q)
            if n == 0:
                yours_0[q] = got.astype(BF16)
                swap_0(q).start()
            else:
                mine[:, pl.ds(q * Q, Q)] = got
                if q:
                    add(q - 1)
        add(NQ - 1)

    def block(i):
        slot = lax.rem(i, 2)
        wait(loads(i, slot))

        @pl.when(i + 1 < NB)
        def _():
            start(loads(i + 1, 1 - slot))

        @pl.when(i == 1)
        def _():
            x_load(0).start()

        @pl.when(i >= 2)
        def _():
            wait(stores(i - 2, slot))

        for t in range(FF // TILE):
            hidden(i, slot, t)
        start(stores(i, slot))

        for t in range(HALF // TILE):
            yours[i, :, pl.ds(t * TILE, TILE)] = term(slot, 1 - core, t, TILE).astype(BF16)
        swap(i).start()
        for t in range(HALF // TILE):
            mine[:, pl.ds(t * TILE, TILE)] = term(slot, core, t, TILE)
        swap(i).wait_recv()
        for n in range(2):
            part = pl.ds(n * HB, HB)
            s_v[2 * i + n] = (mine[part, :] + theirs[i, part, :].astype(F32)).astype(BF16)

            @pl.when(2 * i + n < NX)
            def _():
                cross(2 * i + n).start()

        for k in range(NX, 2 * NB):

            @pl.when(i == k // 2)
            def _():
                start(hand_on(k))

        @pl.when(i <= 2)
        def _():
            finish_0(i - 1)

        @pl.when(i >= 4)
        def _():
            finish(i - 2)

    def step(i, carry):
        block(i)
        return carry

    first_block()
    lax.fori_loop(1, NB, step, 0)

    for j in range(1, NJ):
        x_load(j).start()
    late = {0: (NB - 2,), 1: (NB - 1,), 3: tuple(range(NB, NX))}
    for j in range(NJ):
        x_load(j).wait()
        dw_at(j)[...] = dot(x_at(j)[...], dg_v[...], ((0,), (0,))).astype(BF16)
        dw_store(j).start()
        for k in late.get(j, ()):
            finish(k)

    for i in (NB - 2, NB - 1):
        wait(stores(i, i % 2))
    for i in range(1, NB):
        swap(i).wait_send()
    for k in range(NX, 2 * NB):
        wait(hand_on(k))
    for j in range(NJ):
        dw_store(j).wait()
    for q in range(NQ):
        swap_0(q).wait_send()
        cross_0(q).wait_send()
        keep_0(q).wait()
        give_0(q).wait()
    for k in range(2, NX):
        cross(k).wait_send()
        keep(k).wait()
        give(k).wait()


def terms(dy, gate, up, w_down, w_gate, w_up, x):
    hidden = jax.ShapeDtypeStruct((ROWS, FF), BF16)
    dma = pltpu.SemaphoreType.DMA
    late = 2 * NB - NX
    return pl.pallas_call(
        term_kernel,
        name="terms",
        out_shape=(
            hidden,
            hidden,
            jax.ShapeDtypeStruct((D, FF), BF16),
            jax.ShapeDtypeStruct((2, NX * HB, HALF), BF16),
            *(jax.ShapeDtypeStruct(((b - a) * HB, HALF), BF16) for a, b in PARTS),
            *(jax.ShapeDtypeStruct((2, (b - a) * HB, HALF), BF16) for a, b in PARTS),
        ),
        in_specs=[ANY] * 7,
        out_specs=(ANY,) * (4 + 2 * len(PARTS)),
        scratch_shapes=[
            pltpu.VMEM((FF, D), BF16),
            pltpu.VMEM((D, 2 * FF), BF16),
            pltpu.VMEM((2, RB, D), BF16),
            pltpu.VMEM((2, RB, FF), BF16),
            pltpu.VMEM((2, RB, FF), BF16),
            pltpu.VMEM((2, RB, 2 * FF), BF16),
            pltpu.VMEM((2, RB, FF), BF16),
            pltpu.VMEM((ROWS, FF), BF16),
            pltpu.VMEM((ROWS, BX), BF16),
            pltpu.VMEM((NB, RB, HALF), BF16),
            pltpu.VMEM((RB, HALF), F32),
            pltpu.VMEM((NB, RB, HALF), BF16),
            pltpu.VMEM((2 * NB, HB, HALF), BF16),
            pltpu.VMEM((NX, HB, HALF), BF16),
            pltpu.VMEM((NX, HB, HALF), BF16),
            *(pltpu.VMEM((NQ, RB, Q), BF16) for _ in range(5)),
            dma((FF // TILE,)),
            dma((2, NQ, 2)),
            dma((3, 2)),
            dma((2, 2)),
            dma((NJ,)),
            dma((NJ,)),
            *(dma((NB,)) for _ in range(2)),
            *(dma((NX,)) for _ in range(5)),
            *(dma((late,)) for _ in range(4)),
            *(dma((NQ,)) for _ in range(7)),
        ],
        cost_estimate=pl.CostEstimate(flops=8 * ROWS * D * FF, bytes_accessed=60 * MIB, transcendentals=ROWS * FF),
        compiler_params=pltpu.CompilerParams(collective_id=0, has_side_effects=True, vmem_limit_bytes=62 * MIB),
    )(dy, gate, up, w_down, w_gate, w_up, x)


def weight_kernel(
    x, h, du, dy, dwg_t, dxp, dwg, dwu, dwd, dx,
    x_v, h_v, du_v, dy_v, ou_v, od_v, dwg_v, dx_v, x_sem, h_sem, du_sem, dy_sem, ou_sem, od_sem, take_sem, put_sem,
):
    j = pl.program_id(0)
    slot = lax.rem(j, 2)

    def x_load(j, slot):
        at = pl.ds(pl.multiple_of(j * BX, BX), BX)
        return pltpu.make_async_copy(x.at[:, at], x_v.at[slot], x_sem.at[slot])

    def du_load(t):
        at = pl.ds(t * TILE, TILE)
        return pltpu.make_async_copy(du.at[:, at], du_v.at[:, at], du_sem.at[t])

    def store(src, dst, size, j, sem):
        return pltpu.make_async_copy(src, dst.at[pl.ds(pl.multiple_of(j * size, size), size)], sem)

    def put_up(j, slot):
        return store(ou_v.at[slot], dwu, BX, j, ou_sem.at[slot])

    def put_down(j, slot):
        return store(od_v.at[slot], dwd, BH, j, od_sem.at[slot])

    h_load = pltpu.make_async_copy(h, h_v, h_sem)
    dy_load = pltpu.make_async_copy(dy, dy_v, dy_sem)
    takes = [pltpu.make_async_copy(dxp.at[c], dx_v.at[:, pl.ds(c * HALF, HALF)], take_sem.at[c]) for c in range(2)]
    takes.append(pltpu.make_async_copy(dwg_t, dwg_v, take_sem.at[2]))
    puts = [
        pltpu.make_async_copy(dx_v, dx.at[pl.ds(0, NX * HB)], put_sem.at[0]),
        pltpu.make_async_copy(dwg_v, dwg, put_sem.at[1]),
    ]

    @pl.when(j == 0)
    def _():
        x_load(0, 0).start()
        du_load(0).start()
        x_load(0, 0).wait()
        du_load(1).start()
        for t in range(FF // TILE):
            at = pl.ds(t * TILE, TILE)
            du_load(t).wait()
            if t + 2 < FF // TILE:
                du_load(t + 2).start()
            else:
                if t + 2 == FF // TILE:
                    x_load(1, 1).start()
            ou_v[0, :, at] = dot(x_v[0], du_v[:, at], ((0,), (0,))).astype(BF16)
        put_up(0, 0).start()

    @pl.when(jnp.logical_and(j > 0, j < NJ))
    def _():
        x_load(j, slot).wait()

        @pl.when(j + 1 < NJ)
        def _():
            x_load(j + 1, 1 - slot).start()

        @pl.when(j == 1)
        def _():
            h_load.start()

        @pl.when(j == 2)
        def _():
            dy_load.start()

        @pl.when(j == 3)
        def _():
            for copy in takes:
                copy.start()

        @pl.when(j >= 2)
        def _():
            put_up(j - 2, slot).wait()

        ou_v[slot] = dot(x_v[slot], du_v[...], ((0,), (0,))).astype(BF16)
        put_up(j, slot).start()

    @pl.when(j == NJ)
    def _():
        h_load.wait()
        dy_load.wait()

    @pl.when(j == NJ + 1)
    def _():
        for copy in takes:
            copy.wait()
        for copy in puts:
            copy.start()

    @pl.when(j >= NJ)
    def _():
        k = j - NJ

        @pl.when(k >= 2)
        def _():
            put_down(k - 2, slot).wait()

        od_v[slot] = dot(h_v[:, pl.ds(pl.multiple_of(k * BH, BH), BH)], dy_v[...], ((0,), (0,))).astype(BF16)
        put_down(k, slot).start()

    @pl.when(j == 2 * NJ - 1)
    def _():
        for copy in puts:
            copy.wait()
        for k in (NJ - 2, NJ - 1):
            put_up(k, k % 2).wait()
            put_down(k, k % 2).wait()


def weights(x, h, du, dy, dwg_t, dxp):
    dma = pltpu.SemaphoreType.DMA
    return pl.pallas_call(
        weight_kernel,
        name="weights",
        grid=(2 * NJ,),
        out_shape=(
            jax.ShapeDtypeStruct((D, FF), BF16),
            jax.ShapeDtypeStruct((D, FF), BF16),
            jax.ShapeDtypeStruct((FF, D), BF16),
            jax.ShapeDtypeStruct((ROWS, D), BF16),
        ),
        in_specs=[ANY] * 6,
        out_specs=(ANY,) * 4,
        scratch_shapes=[
            pltpu.VMEM((2, ROWS, BX), BF16),
            pltpu.VMEM((ROWS, FF), BF16),
            pltpu.VMEM((ROWS, FF), BF16),
            pltpu.VMEM((ROWS, D), BF16),
            pltpu.VMEM((2, BX, FF), BF16),
            pltpu.VMEM((2, BH, D), BF16),
            pltpu.VMEM((D, FF), BF16),
            pltpu.VMEM((NX * HB, D), BF16),
            dma((2,)),
            dma,
            dma((FF // TILE,)),
            dma,
            dma((2,)),
            dma((2,)),
            dma((3,)),
            dma((2,)),
        ],
        cost_estimate=pl.CostEstimate(flops=4 * ROWS * D * FF, bytes_accessed=60 * MIB, transcendentals=0),
        compiler_params=pltpu.CompilerParams(vmem_limit_bytes=60 * MIB),
    )(x, h, du, dy, dwg_t, dxp)


def place_kernel(first, both, own, other, dx, out, both_v, own_v, other_v, out_v, in_sem, out_sem):
    core = lax.rem(lax.axis_index("tp"), 2)
    n = own.shape[0] // HB

    def loads(k):
        at = pl.ds(k * HB, HB)
        return [
            pltpu.make_async_copy(both.at[:, at], both_v.at[:, at], in_sem.at[0, k]),
            pltpu.make_async_copy(own.at[at], own_v.at[at], in_sem.at[1, k]),
            pltpu.make_async_copy(other.at[at], other_v.at[at], in_sem.at[2, k]),
        ]

    def store(k):
        return pltpu.make_async_copy(
            out_v.at[pl.ds(k * HB, HB)], out.at[pl.ds((first + k) * HB, HB)], out_sem.at[k]
        )

    for k in range(n):
        for copy in loads(k):
            copy.start()
    for k in range(n):
        at = pl.ds(k * HB, HB)
        for copy in loads(k):
            copy.wait()
        for c in range(2):

            @pl.when(core == c)
            def _():
                for half, q in ((c, own_v), (1 - c, other_v)):
                    total = both_v[half, at].astype(F32) + q[at].astype(F32)
                    out_v[at, half * HALF : (half + 1) * HALF] = total.astype(BF16)

        store(k).start()
    for k in range(n):
        store(k).wait()


def place(dx, both, own, other, first):
    rows = own.shape[0]
    n = rows // HB
    return pl.pallas_call(
        functools.partial(place_kernel, first),
        name="place",
        out_shape=jax.ShapeDtypeStruct(dx.shape, BF16),
        in_specs=[ANY] * 4,
        out_specs=ANY,
        scratch_shapes=[
            pltpu.VMEM((2, rows, HALF), BF16),
            pltpu.VMEM((rows, HALF), BF16),
            pltpu.VMEM((rows, HALF), BF16),
            pltpu.VMEM((rows, D), BF16),
            pltpu.SemaphoreType.DMA((3, n)),
            pltpu.SemaphoreType.DMA((n,)),
        ],
        input_output_aliases={3: 0},
        cost_estimate=pl.CostEstimate(flops=rows * D, bytes_accessed=rows * D * 6, transcendentals=0),
        compiler_params=pltpu.CompilerParams(vmem_limit_bytes=16 * MIB),
    )(both, own, other, dx)


def solution(mesh):
    def step(x, dy, gate, up, w_gate, w_up, w_down):
        du, h, dw_gate, dxp, *parts = terms(dy, gate, up, w_down, w_gate, w_up, x)
        own, both = parts[: len(PARTS)], parts[len(PARTS) :]
        crossed = []
        for part in own:
            crossed.append(lax.ppermute(part, "tp", CHIPS))
        dw_gate, dw_up, dw_down, dx = weights(x, h, du, dy, dw_gate, dxp)
        for (first, _), part, q in zip(PARTS, both, crossed):
            dx, q = lax.optimization_barrier((dx, q))
            near = lax.ppermute(q, "tp", CORES)
            dx = place(dx, part, q, near, first)
        return dx, dw_gate, dw_up, dw_down

    tokens, columns, rows = P("dp", None), P(None, "tp"), P("tp", None)
    return jax.shard_map(
        step,
        mesh=mesh,
        in_specs=(tokens, tokens, P("dp", "tp"), P("dp", "tp"), columns, columns, rows),
        out_specs=(tokens, P("dp", "tp"), P("dp", "tp"), P(("dp", "tp"), None)),
        check_vma=False,
    )
```

```python
import functools

import jax
import jax.numpy as jnp
from jax import lax
from jax.experimental import pallas as pl
from jax.experimental.pallas import tpu as pltpu
from jax.sharding import PartitionSpec as P


MESH = pl.DeviceIdType.MESH
BF16, F32 = jnp.bfloat16, jnp.float32
ANY = pl.BlockSpec(memory_space=pl.ANY)
MIB = 2**20

ROWS, D, FF = 2048, 2048, 1536
HALF = D // 2
RB = 256
NB = ROWS // RB
HB = 64
NP = ROWS // HB
PER = RB // HB
NX = 21
LATE = {0: (12, 13), 1: (14,), 2: (15, 16), 3: (17, 18, 19, 20)}
PARTS = ((21, 27), (27, 32))
TILE = 512
Q = 512
NQ = HALF // Q
BX = 512
NJ = D // BX
BH = FF // NJ

CHIPS = [(0, 2), (2, 0), (1, 3), (3, 1)]
CORES = [(0, 1), (1, 0), (2, 3), (3, 2)]


def dot(a, b, dims):
    return lax.dot_general(a, b, (dims, ((), ())), preferred_element_type=F32)


def to(axis, index):
    return dict(device_id={axis: index}, device_id_type=MESH)


def term_kernel(dy, gate, up, wd, wg, wu, x, du_o, h_o, dwg_o, dxp, *refs):
    n = len(PARTS)
    own_o, both_o, refs = refs[:n], refs[n : 2 * n], refs[2 * n :]
    (
        wd_v, wgu_v, dy_v, ga_v, up_v, dgu_v, h_v, dg_v, x_v, yours, mine, theirs, s_v, q_v, f_v,
        yours_0, theirs_0, s_0, q_0, f_0,
        wd_sem, wg_sem, in_sem, out_sem, x_sem, dw_sem, cs_sem, cr_sem, xs_sem, xr_sem, gs_sem, gr_sem, f_sem,
        own_sem, both_sem, bs_sem, br_sem, cs0, cr0, xs0, xr0, gs0, gr0, f0,
    ) = refs
    me = lax.axis_index("tp")
    core = lax.rem(me, 2)
    partner = me + 1 - 2 * core
    across = lax.rem(me + 2, 4)

    def rows(i):
        return pl.ds(pl.multiple_of(i * RB, RB), RB)

    def loads(i, slot):
        return [
            pltpu.make_async_copy(src.at[rows(i)], dst.at[slot], in_sem.at[n, slot])
            for n, (src, dst) in enumerate(((dy, dy_v), (gate, ga_v), (up, up_v)))
        ]

    def stores(i, slot):
        return [
            pltpu.make_async_copy(dgu_v.at[slot, :, pl.ds(FF, FF)], du_o.at[rows(i)], out_sem.at[0, slot]),
            pltpu.make_async_copy(h_v.at[slot], h_o.at[rows(i)], out_sem.at[1, slot]),
        ]

    def swap(i):
        return pltpu.make_async_remote_copy(
            yours.at[i], theirs.at[i], cs_sem.at[i], cr_sem.at[i], **to("tp", partner)
        )

    def cross(k):
        return pltpu.make_async_remote_copy(s_v.at[k], q_v.at[k], xs_sem.at[k], xr_sem.at[k], **to("tp", across))

    def finished(k):
        return dxp.at[core, pl.ds(pl.multiple_of(k * HB, HB), HB)]

    def keep(k):
        return pltpu.make_async_copy(f_v.at[k], finished(k), f_sem.at[k])

    def give(k):
        return pltpu.make_async_remote_copy(f_v.at[k], finished(k), gs_sem.at[k], gr_sem.at[k], **to("tp", partner))

    def swap_0(q):
        return pltpu.make_async_remote_copy(yours_0.at[q], theirs_0.at[q], cs0.at[q], cr0.at[q], **to("tp", partner))

    def cross_0(q):
        return pltpu.make_async_remote_copy(s_0.at[q], q_0.at[q], xs0.at[q], xr0.at[q], **to("tp", across))

    def finished_0(q):
        return dxp.at[core, pl.ds(0, RB), pl.ds(pl.multiple_of(q * Q, Q), Q)]

    def keep_0(q):
        return pltpu.make_async_copy(f_0.at[q], finished_0(q), f0.at[q])

    def give_0(q):
        return pltpu.make_async_remote_copy(f_0.at[q], finished_0(q), gs0.at[q], gr0.at[q], **to("tp", partner))

    def hand_on(k):
        for own, both, (first, last) in zip(own_o, both_o, PARTS):
            if first <= k < last:
                at, j = pl.ds((k - first) * HB, HB), k - NX
                return (
                    pltpu.make_async_copy(s_v.at[k], own.at[at], own_sem.at[j]),
                    pltpu.make_async_copy(s_v.at[k], both.at[core, at], both_sem.at[j]),
                    pltpu.make_async_remote_copy(
                        s_v.at[k], both.at[core, at], bs_sem.at[j], br_sem.at[j], **to("tp", partner)
                    ),
                )

    def wd_load(t):
        at = pl.ds(t * TILE, TILE)
        return pltpu.make_async_copy(wd.at[at], wd_v.at[at], wd_sem.at[t])

    def wgu_at(half, t, size):
        return pl.ds(pl.multiple_of(half * HALF + t * size, size), size)

    def wgu_load(n, half, t):
        at = wgu_at(half, t, Q)
        return [
            pltpu.make_async_copy(w.at[at], wgu_v.at[at, pl.ds(m * FF, FF)], wg_sem.at[n, t, m])
            for m, w in enumerate((wg, wu))
        ]

    def x_at(j):
        return x_v if j == 0 else wgu_v.at[:, pl.ds((j - 1) * BX, BX)]

    def x_load(j):
        return pltpu.make_async_copy(x.at[:, pl.ds(j * BX, BX)], x_at(j), x_sem.at[j])

    def dw_at(j):
        return wgu_v.at[pl.ds(j * BX, BX), pl.ds(FF, FF)]

    def dw_store(j):
        return pltpu.make_async_copy(dw_at(j), dwg_o.at[pl.ds(j * BX, BX)], dw_sem.at[j])

    def start(copies):
        for copy in copies:
            copy.start()

    def wait(copies):
        for copy in copies:
            copy.wait()

    first_loads = loads(0, 0)
    start([first_loads[0], wd_load(0)])
    start([*first_loads[1:], wd_load(1)])

    barrier = pltpu.get_barrier_semaphore()
    for other in (partner, across):
        pl.semaphore_signal(barrier, inc=1, **to("tp", other))
    pl.semaphore_wait(barrier, 2)

    def finish(k):
        cross(k).wait_recv()
        f_v[k] = (s_v[k].astype(F32) + q_v[k].astype(F32)).astype(BF16)
        keep(k).start()
        give(k).start()

    def finish_0(q):
        cross_0(q).wait_recv()
        f_0[q] = (s_0[q].astype(F32) + q_0[q].astype(F32)).astype(BF16)
        keep_0(q).start()
        give_0(q).start()

    def hidden(i, slot, t):
        cols = pl.ds(t * TILE, TILE)
        d_hidden = dot(dy_v[slot], wd_v[cols, :], ((1,), (1,)))
        if isinstance(i, int) and i == 0 and t == 0:
            wait(first_loads[1:])
        g, u = ga_v[slot, :, cols].astype(F32), up_v[slot, :, cols].astype(F32)
        sig = jax.nn.sigmoid(g)
        silu = g * sig
        d_gate = (d_hidden * u * (sig + silu * (1.0 - sig))).astype(BF16)
        h_v[slot, :, cols] = (silu * u).astype(BF16)
        dgu_v[slot, :, cols] = d_gate
        dg_v[rows(i), cols] = d_gate
        dgu_v[slot, :, pl.ds(FF + t * TILE, TILE)] = (d_hidden * silu).astype(BF16)

    def term(slot, half, t, size):
        return dot(dgu_v[slot], wgu_v[wgu_at(half, t, size), :], ((1,), (1,)))

    def first_block():
        halves = (1 - core, core)
        pieces = [(n, half, q) for q in range(NQ) for n, half in enumerate(halves)]

        def get(n):
            wait(wgu_load(*pieces[n]))
            return term(0, pieces[n][1], pieces[n][2], Q)

        def give_up(q, got):
            yours_0[q] = got.astype(BF16)
            swap_0(q).start()

        def take(q, got):
            mine[:, pl.ds(q * Q, Q)] = got

        def add_0(q):
            swap_0(q).wait_recv()
            s_0[q] = (mine[:, pl.ds(q * Q, Q)] + theirs_0[q].astype(F32)).astype(BF16)
            cross_0(q).start()

        wait([first_loads[0], wd_load(0)])
        start([wd_load(2)])
        hidden(0, 0, 0)
        start(wgu_load(*pieces[0]))
        wait([wd_load(1)])
        hidden(0, 0, 1)
        start(wgu_load(*pieces[1]))
        wait([wd_load(2)])
        hidden(0, 0, 2)
        start(loads(1, 1))
        give_up(0, get(0))
        start(wgu_load(*pieces[2]))
        take(0, get(1))
        start(wgu_load(*pieces[3]))
        wait(loads(1, 1))
        hidden(1, 1, 0)
        add_0(0)
        start(stores(0, 0))
        hidden(1, 1, 1)
        hidden(1, 1, 2)
        give_up(1, get(2))
        start(stores(1, 1))
        start(loads(2, 0))
        take(1, get(3))
        add_0(1)

    def block(i):
        slot = lax.rem(i, 2)

        @pl.when(i + 2 < NB)
        def _():
            start(loads(i + 2, slot))

        @pl.when(i == 1)
        def _():
            x_load(0).start()

        for t in range(HALF // TILE):
            yours[i, :, pl.ds(t * TILE, TILE)] = term(slot, 1 - core, t, TILE).astype(BF16)
        swap(i).start()

        @pl.when(i + 1 < NB)
        def _():
            wait(loads(i + 1, 1 - slot))
            wait(stores(i - 1, 1 - slot))
            for t in range(FF // TILE):
                hidden(i + 1, 1 - slot, t)
            start(stores(i + 1, 1 - slot))

        swap(i).wait_recv()
        for t in range(HALF // TILE):
            cols = pl.ds(t * TILE, TILE)
            total = (term(slot, core, t, TILE) + theirs[i, :, cols].astype(F32)).astype(BF16)
            for n in range(PER):
                s_v[PER * i + n, :, cols] = total[n * HB : (n + 1) * HB]
        for n in range(PER):

            @pl.when(PER * i + n < NX)
            def _():
                cross(PER * i + n).start()

        for k in range(NX, NP):

            @pl.when(i == k // PER)
            def _():
                start(hand_on(k))

        @pl.when(i <= NQ)
        def _():
            finish_0(i - 1)

        @pl.when(i >= 4)
        def _():
            finish(2 * i - 4)
            finish(2 * i - 3)

    def step(i, carry):
        block(i)
        return carry

    first_block()
    lax.fori_loop(1, NB, step, 0)

    for j in range(1, NJ):
        x_load(j).start()
    for j in range(NJ):
        x_load(j).wait()
        dw_at(j)[...] = dot(x_at(j)[...], dg_v[...], ((0,), (0,))).astype(BF16)
        dw_store(j).start()
        for k in LATE[j]:
            finish(k)

    for i in (NB - 2, NB - 1):
        wait(stores(i, i % 2))
    for i in range(1, NB):
        swap(i).wait_send()
    for k in range(NX, NP):
        wait(hand_on(k))
    for j in range(NJ):
        dw_store(j).wait()
    for q in range(NQ):
        swap_0(q).wait_send()
        cross_0(q).wait_send()
        keep_0(q).wait()
        give_0(q).wait()
    for k in range(PER, NX):
        cross(k).wait_send()
        keep(k).wait()
        give(k).wait()


def terms(dy, gate, up, w_down, w_gate, w_up, x):
    hidden = jax.ShapeDtypeStruct((ROWS, FF), BF16)
    dma = pltpu.SemaphoreType.DMA
    late = NP - NX
    return pl.pallas_call(
        term_kernel,
        name="terms",
        out_shape=(
            hidden,
            hidden,
            jax.ShapeDtypeStruct((D, FF), BF16),
            jax.ShapeDtypeStruct((2, NX * HB, HALF), BF16),
            *(jax.ShapeDtypeStruct(((b - a) * HB, HALF), BF16) for a, b in PARTS),
            *(jax.ShapeDtypeStruct((2, (b - a) * HB, HALF), BF16) for a, b in PARTS),
        ),
        in_specs=[ANY] * 7,
        out_specs=(ANY,) * (4 + 2 * len(PARTS)),
        scratch_shapes=[
            pltpu.VMEM((FF, D), BF16),
            pltpu.VMEM((D, 2 * FF), BF16),
            pltpu.VMEM((2, RB, D), BF16),
            pltpu.VMEM((2, RB, FF), BF16),
            pltpu.VMEM((2, RB, FF), BF16),
            pltpu.VMEM((2, RB, 2 * FF), BF16),
            pltpu.VMEM((2, RB, FF), BF16),
            pltpu.VMEM((ROWS, FF), BF16),
            pltpu.VMEM((ROWS, BX), BF16),
            pltpu.VMEM((NB, RB, HALF), BF16),
            pltpu.VMEM((RB, HALF), F32),
            pltpu.VMEM((NB, RB, HALF), BF16),
            pltpu.VMEM((NP, HB, HALF), BF16),
            pltpu.VMEM((NX, HB, HALF), BF16),
            pltpu.VMEM((NX, HB, HALF), BF16),
            *(pltpu.VMEM((NQ, RB, Q), BF16) for _ in range(5)),
            dma((FF // TILE,)),
            dma((2, NQ, 2)),
            dma((3, 2)),
            dma((2, 2)),
            dma((NJ,)),
            dma((NJ,)),
            *(dma((NB,)) for _ in range(2)),
            *(dma((NX,)) for _ in range(5)),
            *(dma((late,)) for _ in range(4)),
            *(dma((NQ,)) for _ in range(7)),
        ],
        cost_estimate=pl.CostEstimate(flops=8 * ROWS * D * FF, bytes_accessed=60 * MIB, transcendentals=ROWS * FF),
        compiler_params=pltpu.CompilerParams(collective_id=0, has_side_effects=True, vmem_limit_bytes=62 * MIB),
    )(dy, gate, up, w_down, w_gate, w_up, x)


def weight_kernel(
    x, h, du, dy, dwg_t, dxp, dwg, dwu, dwd, dx,
    x_v, h_v, du_v, dy_v, ou_v, od_v, dwg_v, dx_v, x_sem, h_sem, du_sem, dy_sem, ou_sem, od_sem, take_sem, put_sem,
):
    j = pl.program_id(0)
    slot = lax.rem(j, 2)

    def x_load(j, slot):
        at = pl.ds(pl.multiple_of(j * BX, BX), BX)
        return pltpu.make_async_copy(x.at[:, at], x_v.at[slot], x_sem.at[slot])

    def du_load(t):
        at = pl.ds(t * TILE, TILE)
        return pltpu.make_async_copy(du.at[:, at], du_v.at[:, at], du_sem.at[t])

    def store(src, dst, size, j, sem):
        return pltpu.make_async_copy(src, dst.at[pl.ds(pl.multiple_of(j * size, size), size)], sem)

    def put_up(j, slot):
        return store(ou_v.at[slot], dwu, BX, j, ou_sem.at[slot])

    def put_down(j, slot):
        return store(od_v.at[slot], dwd, BH, j, od_sem.at[slot])

    h_load = pltpu.make_async_copy(h, h_v, h_sem)
    dy_load = pltpu.make_async_copy(dy, dy_v, dy_sem)
    takes = [pltpu.make_async_copy(dxp.at[c], dx_v.at[:, pl.ds(c * HALF, HALF)], take_sem.at[c]) for c in range(2)]
    takes.append(pltpu.make_async_copy(dwg_t, dwg_v, take_sem.at[2]))
    puts = [
        pltpu.make_async_copy(dx_v, dx.at[pl.ds(0, NX * HB)], put_sem.at[0]),
        pltpu.make_async_copy(dwg_v, dwg, put_sem.at[1]),
    ]

    @pl.when(j == 0)
    def _():
        x_load(0, 0).start()
        du_load(0).start()
        x_load(0, 0).wait()
        du_load(1).start()
        for t in range(FF // TILE):
            at = pl.ds(t * TILE, TILE)
            du_load(t).wait()
            if t + 2 < FF // TILE:
                du_load(t + 2).start()
            else:
                if t + 2 == FF // TILE:
                    x_load(1, 1).start()
            ou_v[0, :, at] = dot(x_v[0], du_v[:, at], ((0,), (0,))).astype(BF16)
        put_up(0, 0).start()

    @pl.when(jnp.logical_and(j > 0, j < NJ))
    def _():
        x_load(j, slot).wait()

        @pl.when(j + 1 < NJ)
        def _():
            x_load(j + 1, 1 - slot).start()

        @pl.when(j == 1)
        def _():
            h_load.start()

        @pl.when(j == 2)
        def _():
            dy_load.start()

        @pl.when(j == 3)
        def _():
            for copy in takes:
                copy.start()

        @pl.when(j >= 2)
        def _():
            put_up(j - 2, slot).wait()

        ou_v[slot] = dot(x_v[slot], du_v[...], ((0,), (0,))).astype(BF16)
        put_up(j, slot).start()

    @pl.when(j == NJ)
    def _():
        h_load.wait()
        dy_load.wait()

    @pl.when(j == NJ + 1)
    def _():
        for copy in takes:
            copy.wait()
        for copy in puts:
            copy.start()

    @pl.when(j >= NJ)
    def _():
        k = j - NJ

        @pl.when(k >= 2)
        def _():
            put_down(k - 2, slot).wait()

        od_v[slot] = dot(h_v[:, pl.ds(pl.multiple_of(k * BH, BH), BH)], dy_v[...], ((0,), (0,))).astype(BF16)
        put_down(k, slot).start()

    @pl.when(j == 2 * NJ - 1)
    def _():
        for copy in puts:
            copy.wait()
        for k in (NJ - 2, NJ - 1):
            put_up(k, k % 2).wait()
            put_down(k, k % 2).wait()


def weights(x, h, du, dy, dwg_t, dxp):
    dma = pltpu.SemaphoreType.DMA
    return pl.pallas_call(
        weight_kernel,
        name="weights",
        grid=(2 * NJ,),
        out_shape=(
            jax.ShapeDtypeStruct((D, FF), BF16),
            jax.ShapeDtypeStruct((D, FF), BF16),
            jax.ShapeDtypeStruct((FF, D), BF16),
            jax.ShapeDtypeStruct((ROWS, D), BF16),
        ),
        in_specs=[ANY] * 6,
        out_specs=(ANY,) * 4,
        scratch_shapes=[
            pltpu.VMEM((2, ROWS, BX), BF16),
            pltpu.VMEM((ROWS, FF), BF16),
            pltpu.VMEM((ROWS, FF), BF16),
            pltpu.VMEM((ROWS, D), BF16),
            pltpu.VMEM((2, BX, FF), BF16),
            pltpu.VMEM((2, BH, D), BF16),
            pltpu.VMEM((D, FF), BF16),
            pltpu.VMEM((NX * HB, D), BF16),
            dma((2,)),
            dma,
            dma((FF // TILE,)),
            dma,
            dma((2,)),
            dma((2,)),
            dma((3,)),
            dma((2,)),
        ],
        cost_estimate=pl.CostEstimate(flops=4 * ROWS * D * FF, bytes_accessed=60 * MIB, transcendentals=0),
        compiler_params=pltpu.CompilerParams(vmem_limit_bytes=60 * MIB),
    )(x, h, du, dy, dwg_t, dxp)


def place_kernel(first, n, both, own, other, dx, out, out_v, sem):
    core = lax.rem(lax.axis_index("tp"), 2)
    rows = own.shape[0] // n

    def store(k):
        return pltpu.make_async_copy(
            out_v.at[pl.ds(k * rows, rows)], out.at[pl.ds(first * HB + k * rows, rows)], sem.at[k]
        )

    for k in range(n):
        at = pl.ds(k * rows, rows)
        for c in range(2):

            @pl.when(core == c)
            def _():
                for half, q in ((c, own), (1 - c, other)):
                    total = both[half, at].astype(F32) + q[at].astype(F32)
                    out_v[at, half * HALF : (half + 1) * HALF] = total.astype(BF16)

        store(k).start()
    for k in range(n):
        store(k).wait()


def place(dx, both, own, other, first, n):
    rows = own.shape[0]
    near = pl.BlockSpec(memory_space=pltpu.VMEM)
    return pl.pallas_call(
        functools.partial(place_kernel, first, n),
        name="place",
        out_shape=jax.ShapeDtypeStruct(dx.shape, BF16),
        in_specs=[near, near, near, ANY],
        out_specs=ANY,
        scratch_shapes=[pltpu.VMEM((rows, D), BF16), pltpu.SemaphoreType.DMA((n,))],
        input_output_aliases={3: 0},
        cost_estimate=pl.CostEstimate(flops=rows * D, bytes_accessed=rows * D * 6, transcendentals=0),
        compiler_params=pltpu.CompilerParams(vmem_limit_bytes=16 * MIB),
    )(both, own, other, dx)


def solution(mesh):
    def step(x, dy, gate, up, w_gate, w_up, w_down):
        du, h, dw_gate, dxp, *parts = terms(dy, gate, up, w_down, w_gate, w_up, x)
        own, both = parts[: len(PARTS)], parts[len(PARTS) :]
        crossed = []
        for part in own:
            crossed.append(lax.ppermute(part, "tp", CHIPS))
        dw_gate, dw_up, dw_down, dx = weights(x, h, du, dy, dw_gate, dxp)
        dx, *crossed = lax.optimization_barrier((dx, *crossed))
        near = []
        for q in crossed:
            near.append(lax.ppermute(q, "tp", CORES))
        for n, (first, _) in enumerate(PARTS):
            dx = place(dx, both[n], crossed[n], near[n], first, 2)
        return dx, dw_gate, dw_up, dw_down

    tokens, columns, rows = P("dp", None), P(None, "tp"), P("tp", None)
    return jax.shard_map(
        step,
        mesh=mesh,
        in_specs=(tokens, tokens, P("dp", "tp"), P("dp", "tp"), columns, columns, rows),
        out_specs=(tokens, P("dp", "tp"), P("dp", "tp"), P(("dp", "tp"), None)),
        check_vma=False,
    )
```

```python
import functools

import jax
import jax.numpy as jnp
from jax import lax
from jax.experimental import pallas as pl
from jax.experimental.pallas import tpu as pltpu
from jax.sharding import PartitionSpec as P


MESH = pl.DeviceIdType.MESH
BF16, F32 = jnp.bfloat16, jnp.float32
ANY = pl.BlockSpec(memory_space=pl.ANY)
MIB = 2**20

ROWS, D, FF = 2048, 2048, 1536
HALF = D // 2
RB = 256
NB = ROWS // RB
HB = 64
NP = ROWS // HB
PER = RB // HB
NX = 21
LATE = {0: (12, 13), 1: (14,), 2: (15, 16), 3: (17, 18, 19, 20)}
PARTS = ((21, 25), (25, 32))
TILE = 512
Q = 512
NQ = HALF // Q
BX = 512
NJ = D // BX
BH = 512
NK = FF // BH

CHIPS = [(0, 2), (2, 0), (1, 3), (3, 1)]
CORES = [(0, 1), (1, 0), (2, 3), (3, 2)]


def dot(a, b, dims):
    return lax.dot_general(a, b, (dims, ((), ())), preferred_element_type=F32)


def to(axis, index):
    return dict(device_id={axis: index}, device_id_type=MESH)


def term_kernel(dy, gate, up, wd, wg, wu, x, du_o, h_o, dwg_o, dxp, *refs):
    n = len(PARTS)
    own_o, both_o, refs = refs[:n], refs[n : 2 * n], refs[2 * n :]
    (
        wd_v, wgu_v, dy_v, ga_v, up_v, dgu_v, h_v, dg_v, x_v, yours, mine, theirs, s_v, q_v, f_v,
        yours_0, theirs_0, s_0, q_0, f_0,
        wd_sem, wg_sem, in_sem, out_sem, x_sem, dw_sem, cs_sem, cr_sem, xs_sem, xr_sem, gs_sem, gr_sem, f_sem,
        own_sem, both_sem, bs_sem, br_sem, cs0, cr0, xs0, xr0, gs0, gr0, f0,
    ) = refs
    me = lax.axis_index("tp")
    core = lax.rem(me, 2)
    partner = me + 1 - 2 * core
    across = lax.rem(me + 2, 4)

    def rows(i):
        return pl.ds(pl.multiple_of(i * RB, RB), RB)

    def loads(i, slot):
        return [
            pltpu.make_async_copy(src.at[rows(i)], dst.at[slot], in_sem.at[n, slot])
            for n, (src, dst) in enumerate(((dy, dy_v), (gate, ga_v), (up, up_v)))
        ]

    def stores(i, slot):
        return [
            pltpu.make_async_copy(dgu_v.at[slot, :, pl.ds(FF, FF)], du_o.at[rows(i)], out_sem.at[0, slot]),
            pltpu.make_async_copy(h_v.at[slot], h_o.at[rows(i)], out_sem.at[1, slot]),
        ]

    def swap(i):
        return pltpu.make_async_remote_copy(
            yours.at[i], theirs.at[i], cs_sem.at[i], cr_sem.at[i], **to("tp", partner)
        )

    def cross(k):
        return pltpu.make_async_remote_copy(s_v.at[k], q_v.at[k], xs_sem.at[k], xr_sem.at[k], **to("tp", across))

    def finished(k):
        return dxp.at[core, pl.ds(pl.multiple_of(k * HB, HB), HB)]

    def keep(k):
        return pltpu.make_async_copy(f_v.at[k], finished(k), f_sem.at[k])

    def give(k):
        return pltpu.make_async_remote_copy(f_v.at[k], finished(k), gs_sem.at[k], gr_sem.at[k], **to("tp", partner))

    def swap_0(q):
        return pltpu.make_async_remote_copy(yours_0.at[q], theirs_0.at[q], cs0.at[q], cr0.at[q], **to("tp", partner))

    def cross_0(q):
        return pltpu.make_async_remote_copy(s_0.at[q], q_0.at[q], xs0.at[q], xr0.at[q], **to("tp", across))

    def finished_0(q):
        return dxp.at[core, pl.ds(0, RB), pl.ds(pl.multiple_of(q * Q, Q), Q)]

    def keep_0(q):
        return pltpu.make_async_copy(f_0.at[q], finished_0(q), f0.at[q])

    def give_0(q):
        return pltpu.make_async_remote_copy(f_0.at[q], finished_0(q), gs0.at[q], gr0.at[q], **to("tp", partner))

    def hand_on(k):
        for own, both, (first, last) in zip(own_o, both_o, PARTS):
            if first <= k < last:
                at, j = pl.ds((k - first) * HB, HB), k - NX
                return (
                    pltpu.make_async_copy(s_v.at[k], own.at[at], own_sem.at[j]),
                    pltpu.make_async_copy(s_v.at[k], both.at[core, at], both_sem.at[j]),
                    pltpu.make_async_remote_copy(
                        s_v.at[k], both.at[core, at], bs_sem.at[j], br_sem.at[j], **to("tp", partner)
                    ),
                )

    def wd_load(t):
        at = pl.ds(t * TILE, TILE)
        return pltpu.make_async_copy(wd.at[at], wd_v.at[at], wd_sem.at[t])

    def wgu_at(half, t, size):
        return pl.ds(pl.multiple_of(half * HALF + t * size, size), size)

    def wgu_load(n, half, t):
        at = wgu_at(half, t, Q)
        return [
            pltpu.make_async_copy(w.at[at], wgu_v.at[at, pl.ds(m * FF, FF)], wg_sem.at[n, t, m])
            for m, w in enumerate((wg, wu))
        ]

    def x_at(j):
        return x_v if j == 0 else wgu_v.at[:, pl.ds((j - 1) * BX, BX)]

    def x_load(j):
        return pltpu.make_async_copy(x.at[:, pl.ds(j * BX, BX)], x_at(j), x_sem.at[j])

    def dw_at(j):
        return wgu_v.at[pl.ds(j * BX, BX), pl.ds(FF, FF)]

    def dw_store(j):
        return pltpu.make_async_copy(dw_at(j), dwg_o.at[pl.ds(j * BX, BX)], dw_sem.at[j])

    def start(copies):
        for copy in copies:
            copy.start()

    def wait(copies):
        for copy in copies:
            copy.wait()

    first_loads = loads(0, 0)
    start([first_loads[0], wd_load(0)])
    start([*first_loads[1:], wd_load(1)])

    barrier = pltpu.get_barrier_semaphore()
    for other in (partner, across):
        pl.semaphore_signal(barrier, inc=1, **to("tp", other))
    pl.semaphore_wait(barrier, 2)

    def finish(k):
        cross(k).wait_recv()
        f_v[k] = (s_v[k].astype(F32) + q_v[k].astype(F32)).astype(BF16)
        keep(k).start()
        give(k).start()

    def finish_0(q):
        cross_0(q).wait_recv()
        f_0[q] = (s_0[q].astype(F32) + q_0[q].astype(F32)).astype(BF16)
        keep_0(q).start()
        give_0(q).start()

    def hidden(i, slot, t):
        cols = pl.ds(t * TILE, TILE)
        d_hidden = dot(dy_v[slot], wd_v[cols, :], ((1,), (1,)))
        if isinstance(i, int) and i == 0 and t == 0:
            wait(first_loads[1:])
        g, u = ga_v[slot, :, cols].astype(F32), up_v[slot, :, cols].astype(F32)
        sig = jax.nn.sigmoid(g)
        silu = g * sig
        d_gate = (d_hidden * u * (sig + silu * (1.0 - sig))).astype(BF16)
        h_v[slot, :, cols] = (silu * u).astype(BF16)
        dgu_v[slot, :, cols] = d_gate
        dg_v[rows(i), cols] = d_gate
        dgu_v[slot, :, pl.ds(FF + t * TILE, TILE)] = (d_hidden * silu).astype(BF16)

    def term(slot, half, t, size):
        return dot(dgu_v[slot], wgu_v[wgu_at(half, t, size), :], ((1,), (1,)))

    def first_block():
        halves = (1 - core, core)
        pieces = [(n, half, q) for q in range(NQ) for n, half in enumerate(halves)]

        def get(n):
            wait(wgu_load(*pieces[n]))
            return term(0, pieces[n][1], pieces[n][2], Q)

        def give_up(q, got):
            yours_0[q] = got.astype(BF16)
            swap_0(q).start()

        def take(q, got):
            mine[:, pl.ds(q * Q, Q)] = got

        def add_0(q):
            swap_0(q).wait_recv()
            s_0[q] = (mine[:, pl.ds(q * Q, Q)] + theirs_0[q].astype(F32)).astype(BF16)
            cross_0(q).start()

        wait([first_loads[0], wd_load(0)])
        start([wd_load(2)])
        hidden(0, 0, 0)
        start(wgu_load(*pieces[0]))
        wait([wd_load(1)])
        hidden(0, 0, 1)
        start(wgu_load(*pieces[1]))
        wait([wd_load(2)])
        hidden(0, 0, 2)
        start(loads(1, 1))
        give_up(0, get(0))
        start(wgu_load(*pieces[2]))
        take(0, get(1))
        start(wgu_load(*pieces[3]))
        wait(loads(1, 1))
        hidden(1, 1, 0)
        add_0(0)
        start(stores(0, 0))
        hidden(1, 1, 1)
        hidden(1, 1, 2)
        give_up(1, get(2))
        start(stores(1, 1))
        start(loads(2, 0))
        take(1, get(3))
        add_0(1)

    def block(i):
        slot = lax.rem(i, 2)

        @pl.when(i + 2 < NB)
        def _():
            start(loads(i + 2, slot))

        @pl.when(i == 1)
        def _():
            x_load(0).start()

        for t in range(HALF // TILE):
            yours[i, :, pl.ds(t * TILE, TILE)] = term(slot, 1 - core, t, TILE).astype(BF16)
        swap(i).start()

        @pl.when(i + 1 < NB)
        def _():
            wait(loads(i + 1, 1 - slot))
            wait(stores(i - 1, 1 - slot))
            for t in range(FF // TILE):
                hidden(i + 1, 1 - slot, t)
            start(stores(i + 1, 1 - slot))

        swap(i).wait_recv()
        for t in range(HALF // TILE):
            cols = pl.ds(t * TILE, TILE)
            total = (term(slot, core, t, TILE) + theirs[i, :, cols].astype(F32)).astype(BF16)
            for n in range(PER):
                s_v[PER * i + n, :, cols] = total[n * HB : (n + 1) * HB]
        for n in range(PER):

            @pl.when(PER * i + n < NX)
            def _():
                cross(PER * i + n).start()

        for k in range(NX, NP):

            @pl.when(i == k // PER)
            def _():
                start(hand_on(k))

        @pl.when(i <= NQ)
        def _():
            finish_0(i - 1)

        @pl.when(i >= 4)
        def _():
            finish(2 * i - 4)
            finish(2 * i - 3)

    def step(i, carry):
        block(i)
        return carry

    first_block()
    lax.fori_loop(1, NB, step, 0)

    for j in range(1, NJ):
        x_load(j).start()
    for j in range(NJ):
        x_load(j).wait()
        dw_at(j)[...] = dot(x_at(j)[...], dg_v[...], ((0,), (0,))).astype(BF16)
        dw_store(j).start()
        for k in LATE[j]:
            finish(k)

    for i in (NB - 2, NB - 1):
        wait(stores(i, i % 2))
    for i in range(1, NB):
        swap(i).wait_send()
    for k in range(NX, NP):
        wait(hand_on(k))
    for j in range(NJ):
        dw_store(j).wait()
    for q in range(NQ):
        swap_0(q).wait_send()
        cross_0(q).wait_send()
        keep_0(q).wait()
        give_0(q).wait()
    for k in range(PER, NX):
        cross(k).wait_send()
        keep(k).wait()
        give(k).wait()


def terms(dy, gate, up, w_down, w_gate, w_up, x):
    hidden = jax.ShapeDtypeStruct((ROWS, FF), BF16)
    dma = pltpu.SemaphoreType.DMA
    late = NP - NX
    return pl.pallas_call(
        term_kernel,
        name="terms",
        out_shape=(
            hidden,
            hidden,
            jax.ShapeDtypeStruct((D, FF), BF16),
            jax.ShapeDtypeStruct((2, NX * HB, HALF), BF16),
            *(jax.ShapeDtypeStruct(((b - a) * HB, HALF), BF16) for a, b in PARTS),
            *(jax.ShapeDtypeStruct((2, (b - a) * HB, HALF), BF16) for a, b in PARTS),
        ),
        in_specs=[ANY] * 7,
        out_specs=(ANY,) * (4 + 2 * len(PARTS)),
        scratch_shapes=[
            pltpu.VMEM((FF, D), BF16),
            pltpu.VMEM((D, 2 * FF), BF16),
            pltpu.VMEM((2, RB, D), BF16),
            pltpu.VMEM((2, RB, FF), BF16),
            pltpu.VMEM((2, RB, FF), BF16),
            pltpu.VMEM((2, RB, 2 * FF), BF16),
            pltpu.VMEM((2, RB, FF), BF16),
            pltpu.VMEM((ROWS, FF), BF16),
            pltpu.VMEM((ROWS, BX), BF16),
            pltpu.VMEM((NB, RB, HALF), BF16),
            pltpu.VMEM((RB, HALF), F32),
            pltpu.VMEM((NB, RB, HALF), BF16),
            pltpu.VMEM((NP, HB, HALF), BF16),
            pltpu.VMEM((NX, HB, HALF), BF16),
            pltpu.VMEM((NX, HB, HALF), BF16),
            *(pltpu.VMEM((NQ, RB, Q), BF16) for _ in range(5)),
            dma((FF // TILE,)),
            dma((2, NQ, 2)),
            dma((3, 2)),
            dma((2, 2)),
            dma((NJ,)),
            dma((NJ,)),
            *(dma((NB,)) for _ in range(2)),
            *(dma((NX,)) for _ in range(5)),
            *(dma((late,)) for _ in range(4)),
            *(dma((NQ,)) for _ in range(7)),
        ],
        cost_estimate=pl.CostEstimate(flops=8 * ROWS * D * FF, bytes_accessed=60 * MIB, transcendentals=ROWS * FF),
        compiler_params=pltpu.CompilerParams(collective_id=0, has_side_effects=True, vmem_limit_bytes=62 * MIB),
    )(dy, gate, up, w_down, w_gate, w_up, x)


def weight_kernel(
    x, h, du, dy, dwg_t, dxp, dwg, dwu, dwd, dx,
    x_v, h_v, du_v, dy_v, ou_v, od_v, dwg_v, dx_v, x_sem, h_sem, du_sem, dy_sem, ou_sem, od_sem, take_sem, put_sem,
):
    j = pl.program_id(0)
    slot = lax.rem(j, 2)

    def x_load(j, slot):
        at = pl.ds(pl.multiple_of(j * BX, BX), BX)
        return pltpu.make_async_copy(x.at[:, at], x_v.at[slot], x_sem.at[slot])

    def du_load(t):
        at = pl.ds(t * TILE, TILE)
        return pltpu.make_async_copy(du.at[:, at], du_v.at[:, at], du_sem.at[t])

    def store(src, dst, size, j, sem):
        return pltpu.make_async_copy(src, dst.at[pl.ds(pl.multiple_of(j * size, size), size)], sem)

    def put_up(j, slot):
        return store(ou_v.at[slot], dwu, BX, j, ou_sem.at[slot])

    def put_down(j, slot):
        return store(od_v.at[slot], dwd, BH, j, od_sem.at[slot])

    h_load = pltpu.make_async_copy(h, h_v, h_sem)
    dy_load = pltpu.make_async_copy(dy, dy_v, dy_sem)
    takes = [pltpu.make_async_copy(dxp.at[c], dx_v.at[:, pl.ds(c * HALF, HALF)], take_sem.at[c]) for c in range(2)]
    takes.append(pltpu.make_async_copy(dwg_t, dwg_v, take_sem.at[2]))
    puts = [
        pltpu.make_async_copy(dx_v, dx.at[pl.ds(0, NX * HB)], put_sem.at[0]),
        pltpu.make_async_copy(dwg_v, dwg, put_sem.at[1]),
    ]

    @pl.when(j == 0)
    def _():
        x_load(0, 0).start()
        du_load(0).start()
        x_load(0, 0).wait()
        du_load(1).start()
        for t in range(FF // TILE):
            at = pl.ds(t * TILE, TILE)
            du_load(t).wait()
            if t + 2 < FF // TILE:
                du_load(t + 2).start()
            else:
                if t + 2 == FF // TILE:
                    x_load(1, 1).start()
            ou_v[0, :, at] = dot(x_v[0], du_v[:, at], ((0,), (0,))).astype(BF16)
        put_up(0, 0).start()

    @pl.when(jnp.logical_and(j > 0, j < NJ))
    def _():
        x_load(j, slot).wait()

        @pl.when(j + 1 < NJ)
        def _():
            x_load(j + 1, 1 - slot).start()

        @pl.when(j == 1)
        def _():
            h_load.start()

        @pl.when(j == 2)
        def _():
            dy_load.start()

        @pl.when(j == 3)
        def _():
            for copy in takes:
                copy.start()

        @pl.when(j >= 2)
        def _():
            put_up(j - 2, slot).wait()

        ou_v[slot] = dot(x_v[slot], du_v[...], ((0,), (0,))).astype(BF16)
        put_up(j, slot).start()

    @pl.when(j == NJ)
    def _():
        h_load.wait()
        dy_load.wait()

    @pl.when(j == NJ + 1)
    def _():
        for copy in takes:
            copy.wait()
        for copy in puts:
            copy.start()

    @pl.when(j >= NJ)
    def _():
        k = j - NJ

        @pl.when(k >= 2)
        def _():
            put_down(k - 2, slot).wait()

        od_v[slot] = dot(h_v[:, pl.ds(pl.multiple_of(k * BH, BH), BH)], dy_v[...], ((0,), (0,))).astype(BF16)
        put_down(k, slot).start()

    @pl.when(j == NJ + NK - 1)
    def _():
        for copy in puts:
            copy.wait()
        for k in (NJ - 2, NJ - 1):
            put_up(k, k % 2).wait()
        for k in (NK - 2, NK - 1):
            put_down(k, k % 2).wait()


def weights(x, h, du, dy, dwg_t, dxp):
    dma = pltpu.SemaphoreType.DMA
    return pl.pallas_call(
        weight_kernel,
        name="weights",
        grid=(NJ + NK,),
        out_shape=(
            jax.ShapeDtypeStruct((D, FF), BF16),
            jax.ShapeDtypeStruct((D, FF), BF16),
            jax.ShapeDtypeStruct((FF, D), BF16),
            jax.ShapeDtypeStruct((ROWS, D), BF16),
        ),
        in_specs=[ANY] * 6,
        out_specs=(ANY,) * 4,
        scratch_shapes=[
            pltpu.VMEM((2, ROWS, BX), BF16),
            pltpu.VMEM((ROWS, FF), BF16),
            pltpu.VMEM((ROWS, FF), BF16),
            pltpu.VMEM((ROWS, D), BF16),
            pltpu.VMEM((2, BX, FF), BF16),
            pltpu.VMEM((2, BH, D), BF16),
            pltpu.VMEM((D, FF), BF16),
            pltpu.VMEM((NX * HB, D), BF16),
            dma((2,)),
            dma,
            dma((FF // TILE,)),
            dma,
            dma((2,)),
            dma((2,)),
            dma((3,)),
            dma((2,)),
        ],
        cost_estimate=pl.CostEstimate(flops=4 * ROWS * D * FF, bytes_accessed=60 * MIB, transcendentals=0),
        compiler_params=pltpu.CompilerParams(vmem_limit_bytes=52 * MIB),
    )(x, h, du, dy, dwg_t, dxp)


def place_kernel(first, n, both, own, other, dx, out, out_v, sem):
    core = lax.rem(lax.axis_index("tp"), 2)
    rows = own.shape[0] // n

    def store(k):
        return pltpu.make_async_copy(
            out_v.at[pl.ds(k * rows, rows)], out.at[pl.ds(first * HB + k * rows, rows)], sem.at[k]
        )

    for k in range(n):
        at = pl.ds(k * rows, rows)
        for c in range(2):

            @pl.when(core == c)
            def _():
                for half, q in ((c, own), (1 - c, other)):
                    total = both[half, at].astype(F32) + q[at].astype(F32)
                    out_v[at, half * HALF : (half + 1) * HALF] = total.astype(BF16)

        store(k).start()
    for k in range(n):
        store(k).wait()


def place(dx, both, own, other, first, n):
    rows = own.shape[0]
    near = pl.BlockSpec(memory_space=pltpu.VMEM)
    return pl.pallas_call(
        functools.partial(place_kernel, first, n),
        name="place",
        out_shape=jax.ShapeDtypeStruct(dx.shape, BF16),
        in_specs=[near, near, near, ANY],
        out_specs=ANY,
        scratch_shapes=[pltpu.VMEM((rows, D), BF16), pltpu.SemaphoreType.DMA((n,))],
        input_output_aliases={3: 0},
        cost_estimate=pl.CostEstimate(flops=rows * D, bytes_accessed=rows * D * 6, transcendentals=0),
        compiler_params=pltpu.CompilerParams(vmem_limit_bytes=16 * MIB),
    )(both, own, other, dx)


def solution(mesh):
    def step(x, dy, gate, up, w_gate, w_up, w_down):
        du, h, dw_gate, dxp, *parts = terms(dy, gate, up, w_down, w_gate, w_up, x)
        own, both = parts[: len(PARTS)], parts[len(PARTS) :]
        crossed = []
        for part in own:
            crossed.append(lax.ppermute(part, "tp", CHIPS))
        dw_gate, dw_up, dw_down, dx = weights(x, h, du, dy, dw_gate, dxp)
        dx, *crossed = lax.optimization_barrier((dx, *crossed))
        near = []
        for q in crossed:
            near.append(lax.ppermute(q, "tp", CORES))
        for n, (first, _) in enumerate(PARTS):
            dx = place(dx, both[n], crossed[n], near[n], first, 2)
        return dx, dw_gate, dw_up, dw_down

    tokens, columns, rows = P("dp", None), P(None, "tp"), P("tp", None)
    return jax.shard_map(
        step,
        mesh=mesh,
        in_specs=(tokens, tokens, P("dp", "tp"), P("dp", "tp"), columns, columns, rows),
        out_specs=(tokens, P("dp", "tp"), P("dp", "tp"), P(("dp", "tp"), None)),
        check_vma=False,
    )
```
